32 devices in a mesh: dp: 4 (over z), seq: 8 (over y, x, core).
Axes of the slice: x: 2, y: 2, z: 4, core: 2. Of those that a mesh axis runs over, the one named last changes fastest.
Arguments:
- projections: bfloat16 [1, 4, 1024, 4096], P(None, 'dp', 'seq'), may hold values from -6 to 6
- rotated_query_gradient: bfloat16 [1, 4, 1024, 4096], P(None, 'dp', None, 'seq'), may hold values from -6 to 6
- gains: float32 [1, 4096], replicated, may hold values from 0.25 to 1.75
- adapter_lowering: bfloat16 [1, 48, 5120], P(None, 'dp'), may hold values from -0.078125 to 0.078125
- adapter_raising: bfloat16 [1, 48, 4096], P(None, 'dp'), may hold values from -0.875 to 0.875
- activations: bfloat16 [4, 1024, 5120], P('dp', 'seq'), may hold values from -6 to 6
- positions: int32 [3, 4, 1024], P(None, 'dp', 'seq'), may hold values from 0 to 22, as said below
- valid: int32 [4, 1024], P('dp', 'seq'), may hold values from 0 to 1, as said below
Outputs:
- grad_down: float32 [1, 48, 5120], P(None, 'dp')
- grad_up: float32 [1, 48, 4096], P(None, 'dp')
- grad_gain: float32 [1, 4096], replicated
The draws below stay inside these ranges and needn't reach their ends.
Inputs may be any that keep to these rules, and one draw needn't show every extreme that they name: `positions`: within a video the frame index never falls; one frame holds 128 tokens. Every eighth token of a video is valid.
All inputs are finite; a program needn't handle non-finite values.
Results may differ from the reference program's by a relative error of at most 0.0041.
Values may be sent and summed in bfloat16 or wider, within the bound.
A program may use at most 64 MiB of HBM per device.

```python
import jax
import jax.numpy as jnp
from jax import lax

MODEL_WIDTH = 5120
HD = 128
ADAPTER_RANK = 48
QUERY_FEATURES = 4096
LEN = 1024
SAMPLES = 4


def draw_positions(key, part):
    token_index = jnp.arange(LEN, dtype=jnp.int32)
    offsets = jax.random.randint(key, (3, SAMPLES, 1), 0, 8)
    sample_index = jnp.arange(SAMPLES, dtype=jnp.int32)[None, :, None]
    offsets = jnp.where(sample_index == 0, 0, offsets)
    offsets = jnp.where(sample_index == SAMPLES - 1, 7, offsets)
    grid_base = jnp.stack([token_index // 128, token_index // 16 % 8, token_index % 16])[:, None, :]
    return (grid_base + offsets).astype(jnp.int32)


def draw_valid(key, part):
    token_index = jnp.arange(LEN, dtype=jnp.int32)
    draw_level = jax.random.randint(key, (SAMPLES, LEN), 0, 1000)
    kept_rows = draw_level < 300 + 600 * token_index // LEN
    return jnp.where((token_index % 8 == 0) | kept_rows, 1, 0).astype(jnp.int32)


def levels(rng, extent, shards, least, largest):
    gain = 1.0
    for dim, blocks in shards:
        heights = jax.random.uniform(jax.random.fold_in(jax.random.fold_in(rng, 6), dim), (blocks,), jnp.float32, least / len(shards), largest / len(shards))
        gain = gain * jnp.repeat(jnp.exp(heights), extent[dim] // blocks).reshape((-1,) + (1,) * (len(extent) - 1 - dim))
    return gain


def noise(key, dims, spread, bound, cuts=(), held_as=jnp.bfloat16):
    values = jax.random.normal(key, dims, jnp.float32) * spread
    if len(cuts) > 0:
        values = levels(key, dims, cuts, -0.22, 0.18) * values
    return jnp.clip(values, min=-bound, max=bound).astype(held_as)


def setup_inputs(seed: int = 0) -> dict:
    seeds = jax.random.split(jax.random.key(seed), 9)
    projections = noise(seeds[0], (1, SAMPLES, LEN, QUERY_FEATURES), 1.0, 6.0, ((1, 4), (2, 8)))
    rotated_query_gradient = noise(seeds[1], (1, SAMPLES, LEN, QUERY_FEATURES), 1.0, 6.0, ((1, 4), (3, 8)))
    gains = jnp.clip(1.0 + 0.15 * jax.random.normal(seeds[2], (1, QUERY_FEATURES), jnp.float32), 0.25, 1.75)
    adapter_lowering = noise(seeds[3], (1, ADAPTER_RANK, MODEL_WIDTH), MODEL_WIDTH ** -0.5, 0.078125, ((1, 4),))
    adapter_raising = noise(seeds[4], (1, ADAPTER_RANK, QUERY_FEATURES), ADAPTER_RANK ** -0.5, 0.875, ((1, 4),))
    activations = noise(seeds[5], (SAMPLES, LEN, MODEL_WIDTH), 1.0, 6.0, ((0, 4), (1, 8)))
    positions = draw_positions(jax.random.fold_in(seeds[8], 71), 0)
    valid = draw_valid(jax.random.fold_in(seeds[8], 71), 0)
    return {"projections": projections, "rotated_query_gradient": rotated_query_gradient, "gains": gains, "adapter_lowering": adapter_lowering, "adapter_raising": adapter_raising, "activations": activations, "positions": positions, "valid": valid}


EPSILON = 1e-06

def rope_tables(positions, head_size):
    one_sixth = head_size // 6
    counts = (head_size // 2 - 2 * one_sixth, one_sixth, one_sixth)
    pieces = []
    for component in range(3):
        frequency = 10000.0 ** (-jnp.arange(counts[component], dtype=jnp.float32) / counts[component])
        pieces.append(positions[component].astype(jnp.float32)[..., None] * frequency)
    angles = jnp.concatenate(pieces, -1)
    return (jnp.cos(angles), jnp.sin(angles))

def norm_backward(projections, rotated_query_gradient, gains, positions, valid):
    cosine, sine_table = rope_tables(positions, HD)
    full_shape = rotated_query_gradient.shape
    cotangent = rotated_query_gradient.astype(jnp.float32) * valid.astype(jnp.float32)[None, :, :, None]
    cotangent = cotangent.reshape(full_shape[:3] + (full_shape[3] // HD, HD // 2, 2))
    cosine = cosine[None, :, :, None, :]
    sine_table = sine_table[None, :, :, None, :]
    even_part = cosine * cotangent[..., 0] + sine_table * cotangent[..., 1]
    odd_part = cosine * cotangent[..., 1] - sine_table * cotangent[..., 0]
    unrotated = jnp.stack([even_part, odd_part], -1).reshape(full_shape)
    values = projections.astype(jnp.float32)
    inverse = lax.rsqrt(lax.optimization_barrier(jnp.mean(values * values, -1, keepdims=True)) + EPSILON)
    normed = values * inverse
    gain_part = lax.optimization_barrier(jnp.sum(unrotated * normed, axis=(1, 2)))
    scaled = unrotated * gains[:, None, None, :]
    projection_change = inverse * (scaled - normed * lax.optimization_barrier(jnp.mean(scaled * normed, -1, keepdims=True)))
    return (projection_change.astype(jnp.bfloat16), gain_part)

def adapter_partial_terms(projection_change, input_list, lowering_matrices, raising_matrices):
    down_terms = []
    up_terms = []
    for member in range(projection_change.shape[0]):
        reduced = jnp.dot(input_list, lowering_matrices[member].T, preferred_element_type=jnp.float32).astype(jnp.bfloat16)
        up_terms.append(jnp.dot(reduced.T, projection_change[member], preferred_element_type=jnp.float32))
        back_rank = jnp.dot(projection_change[member], raising_matrices[member].T, preferred_element_type=jnp.float32).astype(jnp.bfloat16)
        down_terms.append(jnp.dot(back_rank.T, input_list, preferred_element_type=jnp.float32))
    return (jnp.stack(down_terms), jnp.stack(up_terms))

def reference(projections, rotated_query_gradient, gains, adapter_lowering, adapter_raising, activations, positions, valid):
    count = jnp.sum(valid.astype(jnp.float32))
    factor = SAMPLES * LEN / count

    def one_sample(items):
        proj_one, grad_one, pos_one, valid_one, single_input = items
        projection_change, gain_part = norm_backward(proj_one[:, None], grad_one[:, None], gains, pos_one[:, None], valid_one[None])
        lowering_portion, raising_portion = adapter_partial_terms(projection_change[:, 0], single_input, adapter_lowering, adapter_raising)
        return (lowering_portion, raising_portion, gain_part)
    down_all, up_all, gain_all = lax.map(one_sample, (jnp.moveaxis(projections, 1, 0), jnp.moveaxis(rotated_query_gradient, 1, 0), jnp.moveaxis(positions, 1, 0), valid, activations))
    return (factor * lax.optimization_barrier(jnp.sum(down_all, 0)), factor * lax.optimization_barrier(jnp.sum(up_all, 0)), factor * lax.optimization_barrier(jnp.sum(gain_all, 0)))
```

```python
import functools

import jax
import jax.numpy as jnp
import numpy as np
from jax import lax
from jax.experimental import pallas as pl
from jax.experimental.pallas import tpu as pltpu
from jax.sharding import PartitionSpec as P

HD = 128
EPSILON = 1e-06
LANES = 128
BF = jnp.bfloat16
F32 = jnp.float32
MESH = pl.DeviceIdType.MESH
NT = (((1,), (1,)), ((), ()))


def group_counts():
    one_sixth = HD // 6
    return (HD // 2 - 2 * one_sixth, one_sixth, one_sixth)


def lane_frequencies():
    pieces = []
    for n in group_counts():
        pieces.append(np.float32(10000.0) ** (-np.arange(n, dtype=np.float32) / np.float32(n)))
    return np.repeat(np.concatenate(pieces).astype(np.float32), 2)[None]


def kernel(
    cfg,
    proj_hbm, cot_hbm, act_hbm, adapt_hbm, gains_ref, freq_ref, pos_ref, valid_ref,
    down_ref, up_ref, gain_ref,
    proj, act, cot, adapt, scaled, back_acc, dot_acc, inv_ref, cos_ref, sin_ref, redt, backt,
    small_send, small_recv, small_dp, small_dp_recv, small_fin, small_ag,
    d2d_send_u, d2d_recv_u, own_u, rs_send_u, rs_recv_u, tot_u, dp_send_u, dp_f_u, dp_recv_u, ag_u, fin_u,
    d2d_send_d, d2d_recv_d, own_d, rs_send_d, rs_recv_d, tot_d, dp_send_d, dp_f_d, dp_recv_d, ag_d, fin_d,
    local_sem, cot_s, cot_r, ad_s, ad_r, rel_s, rel_r,
    sm_s, sm_r, smd_s, smd_r, sma_s, sma_r,
    d2d_s, d2d_r, rs_s, rs_r, dp_s, dp_r, ag_s, ag_r,
):
    S, D, T, F, W, R, RP, LH, M, QF = (
        cfg[k] for k in ("S", "D", "T", "F", "W", "R", "RP", "LH", "M", "QF")
    )
    K = S // 2
    ranks = D * R
    hw = 256 if F % 256 == 0 else 128
    d = lax.axis_index("dp")
    s = lax.axis_index("seq")
    c = lax.rem(s, 2)
    chip = s // 2
    sib = s + 1 - 2 * c

    def copy(src, dst, ss, rs, dp, seq):
        return pltpu.make_async_remote_copy(
            src_ref=src, dst_ref=dst, send_sem=ss, recv_sem=rs,
            device_id=(dp, seq), device_id_type=MESH,
        )

    loads = [
        pltpu.make_async_copy(proj_hbm, proj, local_sem.at[0]),
        pltpu.make_async_copy(act_hbm, act.at[:, pl.ds(0, M)], local_sem.at[1]),
        pltpu.make_async_copy(cot_hbm.at[s], cot.at[s], local_sem.at[2]),
        pltpu.make_async_copy(adapt_hbm, adapt.at[d], local_sem.at[3]),
    ]
    for x in loads:
        x.start()

    barrier = pltpu.get_barrier_semaphore()
    for k in range(1, S):
        pl.semaphore_signal(barrier, inc=1, device_id=(d, lax.rem(s + k, S)), device_id_type=MESH)
    for k in range(1, D):
        pl.semaphore_signal(barrier, inc=1, device_id=(lax.rem(d + k, D), s), device_id_type=MESH)
    pl.semaphore_wait(barrier, S + D - 2)

    def cot_copy(peer, slot):
        return copy(cot_hbm.at[peer], cot.at[slot], cot_s.at[peer], cot_r.at[slot], d, peer)

    def adapt_copy(peer, slot):
        return copy(adapt_hbm.at[c], adapt.at[slot, c], ad_s.at[peer], ad_r.at[slot], peer, s)

    def relay_copy(slot, half):
        return copy(adapt.at[slot, half], adapt.at[slot, half], rel_s.at[slot], rel_r.at[slot], d, sib)

    for k in range(1, D):
        adapt_copy(lax.rem(d + k, D), d).start()
    for k in range(1, S):
        cot_copy(lax.rem(s + k, S), s).start()

    n0, n1, _ = group_counts()
    lane = lax.broadcasted_iota(jnp.int32, (T, LANES), 1)

    def column(row):
        return jnp.broadcast_to(row.astype(F32), (LANES, T)).T

    index = jnp.where(
        lane < 2 * n0, column(pos_ref[0:1, :]),
        jnp.where(lane < 2 * (n0 + n1), column(pos_ref[1:2, :]), column(pos_ref[2:3, :])),
    )
    angle = index * freq_ref[...]
    ok = column(valid_ref[...])
    co = jnp.cos(angle) * ok
    si = jnp.sin(angle) * ok
    for i in range(hw // LANES):
        cos_ref[:, i * LANES:(i + 1) * LANES] = co
        sin_ref[:, i * LANES:(i + 1) * LANES] = si
    row_i = lax.broadcasted_iota(jnp.int32, (hw, hw), 0)
    col_i = lax.broadcasted_iota(jnp.int32, (hw, hw), 1)
    even = lax.rem(col_i, 2) == 0
    swap = jnp.where(
        even & (row_i == col_i + 1), 1.0, jnp.where(jnp.logical_not(even) & (row_i == col_i - 1), -1.0, 0.0)
    ).astype(BF)
    count = jnp.sum(valid_ref[...].astype(F32), axis=1, keepdims=True)
    small_send[...] = jnp.broadcast_to(count[:, :, None], small_send.shape)

    loads[0].wait()
    square = jnp.zeros((T, LANES), F32)
    for i in range(QF // LANES):
        v = proj[:, i * LANES:(i + 1) * LANES].astype(F32)
        square += v * v
    inverse = lax.rsqrt(jnp.sum(square, axis=1, keepdims=True) / QF + EPSILON)
    inv_ref[...] = jnp.broadcast_to(inverse, (T, LANES))
    dot_acc[...] = jnp.zeros_like(dot_acc)

    def wide(x):
        return jnp.concatenate([x] * (hw // LANES), axis=1) if hw > LANES else x

    def chunk(p):
        inv = wide(inv_ref[...])
        cw, sw = cos_ref[...], sin_ref[...]
        for i in range(F // hw):
            cols = pl.ds(pl.multiple_of(p * F + i * hw, LANES), hw)
            x = cot[p, :, i * hw:(i + 1) * hw]
            xs = jnp.dot(x, swap, preferred_element_type=F32)
            un = cw * x.astype(F32) + sw * xs
            prod = un * (proj[:, cols].astype(F32) * inv)
            g = jnp.sum(prod, axis=0, keepdims=True)
            for t in range(hw // LANES):
                j = i * (hw // LANES) + t
                small_send[p, j:j + 1, :] = g[:, t * LANES:(t + 1) * LANES]
            gn = gains_ref[:, cols]
            scaled[p, :, i * hw:(i + 1) * hw] = un * gn
            pg = prod * gn
            acc = pg[:, :LANES]
            for t in range(1, hw // LANES):
                acc += pg[:, t * LANES:(t + 1) * LANES]
            dot_acc[...] += acc

    loads[2].wait()
    chunk(s)
    cot_copy(sib, sib).wait_recv()
    chunk(sib)
    loads[3].wait()

    def rest(j, carry):
        p = lax.rem(2 * chip + 2 + j, S)
        cot_copy(p, p).wait_recv()
        chunk(p)
        return carry

    half_rest = (S - 2) // 2
    lax.fori_loop(0, half_rest, rest, 0)
    for k in range(1, D):
        e = lax.rem(d + k, D)
        adapt_copy(e, e).wait_recv()
        relay_copy(e, c).start()
    lax.fori_loop(half_rest, S - 2, rest, 0)

    def small_copy(peer, slot):
        return copy(small_send.at[peer], small_recv.at[slot], sm_s.at[peer], sm_r.at[slot], d, peer)

    for k in range(1, S):
        small_copy(lax.rem(s + k, S), s).start()

    r_i = lax.broadcasted_iota(jnp.int32, (ranks, D * RP), 0)
    q_i = lax.broadcasted_iota(jnp.int32, (ranks, D * RP), 1)
    pick = jnp.where(q_i == (r_i // R) * RP + lax.rem(r_i, R), 1.0, 0.0).astype(BF)

    def dense_transposed(x):
        return lax.dot_general(pick, x.astype(BF), NT, preferred_element_type=F32).astype(BF)

    for k in range(1, D):
        e = lax.rem(d + k, D)
        relay_copy(e, 1 - c).wait_recv()
    loads[1].wait()
    red = jnp.zeros((T, D * RP), F32)
    for h in range(2):
        low = adapt[:, h, :, 0:LH].reshape(D * RP, LH)
        red += lax.dot_general(act[:, h * LH:(h + 1) * LH], low, NT, preferred_element_type=F32)
    redt[...] = dense_transposed(red)

    back_acc[...] = jnp.zeros_like(back_acc)
    dot_mean = jnp.sum(dot_acc[...], axis=1, keepdims=True) / QF
    mean_w = jnp.broadcast_to(dot_mean, (T, LANES))
    dot_acc[...] = mean_w

    def up_term(p):
        inv = wide(inv_ref[...])
        mean = wide(dot_acc[...])
        parts = []
        for i in range(F // hw):
            cols = pl.ds(pl.multiple_of(p * F + i * hw, LANES), hw)
            nrm = proj[:, cols].astype(F32) * inv
            parts.append((inv * (scaled[p, :, i * hw:(i + 1) * hw] - nrm * mean)).astype(BF))
        delta = jnp.concatenate(parts, axis=1) if len(parts) > 1 else parts[0]
        h = p // K
        off = pl.multiple_of(LH + lax.rem(p, K) * F, LANES)
        rai = adapt[:, h, :, pl.ds(off, F)].reshape(D * RP, F)
        back_acc[...] += lax.dot_general(delta, rai, NT, preferred_element_type=F32)
        return jnp.dot(redt[...], delta, preferred_element_type=F32)

    def down_term(p):
        cols = pl.ds(pl.multiple_of(p * W, LANES), W)
        return jnp.dot(backt[...], act[:, cols], preferred_element_type=F32)

    up = dict(i=0, term=up_term, d2d_send=d2d_send_u, d2d_recv=d2d_recv_u, own=own_u,
              rs_send=rs_send_u, rs_recv=rs_recv_u, tot=tot_u, dp_send=dp_send_u, dp_f=dp_f_u,
              dp_recv=dp_recv_u, ag=ag_u, fin=fin_u, out=up_ref, width=F)
    down = dict(i=1, term=down_term, d2d_send=d2d_send_d, d2d_recv=d2d_recv_d, own=own_d,
                rs_send=rs_send_d, rs_recv=rs_recv_d, tot=tot_d, dp_send=dp_send_d, dp_f=dp_f_d,
                dp_recv=dp_recv_d, ag=ag_d, fin=fin_d, out=down_ref, width=W)

    def d2d_copy(b, k):
        i = b["i"]
        return copy(b["d2d_send"].at[k], b["d2d_recv"].at[k], d2d_s.at[i, k], d2d_r.at[i, k], d, sib)

    def rs_copy(b, peer, slot):
        i = b["i"]
        return copy(b["rs_send"].at[peer], b["rs_recv"].at[slot], rs_s.at[i, peer], rs_r.at[i, slot],
                    d, 2 * peer + c)

    def dp_copy(b, peer, slot):
        i = b["i"]
        return copy(b["dp_send"].at[peer], b["dp_recv"].at[slot], dp_s.at[i, peer], dp_r.at[i, slot],
                    peer, s)

    def ag_copy(b, peer, slot):
        i = b["i"]
        return copy(b["fin"], b["ag"].at[slot], ag_s.at[i, peer], ag_r.at[i, slot], d, peer)

    def scatter(b):
        def for_sibling(j, carry):
            k = lax.rem(chip + 1 + j, K)
            b["d2d_send"][k] = b["term"](2 * k + 1 - c).astype(BF)
            d2d_copy(b, k).start()
            return carry

        def for_this_core(j, carry):
            k = lax.rem(chip + 1 + j, K)
            b["own"][k] = b["term"](2 * k + c)
            return carry

        lax.fori_loop(0, K, for_sibling, 0)
        lax.fori_loop(0, K, for_this_core, 0)
        for j in range(1, K):
            k = lax.rem(chip + j, K)
            d2d_copy(b, k).wait_recv()
            b["rs_send"][k] = (b["own"][k] + b["d2d_recv"][k].astype(F32)).astype(BF)
            rs_copy(b, k, chip).start()

    def dp_stage(b):
        d2d_copy(b, chip).wait_recv()
        total = b["own"][chip] + b["d2d_recv"][chip].astype(F32)
        for j in range(1, K):
            q = lax.rem(chip + j, K)
            rs_copy(b, q, q).wait_recv()
            total += b["rs_recv"][q].astype(F32)
        b["tot"][0:ranks, :] = total
        for e in range(D):
            rows = b["tot"][e * R:e * R + RP, :]
            b["dp_f"][e] = rows
            b["dp_send"][e] = rows.astype(BF)
        for k in range(1, D):
            dp_copy(b, lax.rem(d + k, D), d).start()

    def gather(b, factor):
        total = b["dp_f"][d]
        for k in range(1, D):
            e = lax.rem(d + k, D)
            dp_copy(b, e, e).wait_recv()
            total += b["dp_recv"][e].astype(F32)
        fin = (total * factor).astype(BF)
        b["fin"][...] = fin
        for k in range(1, S):
            ag_copy(b, lax.rem(s + k, S), s).start()
        cols = pl.ds(pl.multiple_of(s * b["width"], LANES), b["width"])
        b["out"][:, cols] = fin.astype(F32)[0:R]

    scatter(up)

    small = small_send[s]
    for k in range(1, S):
        q = lax.rem(s + k, S)
        small_copy(q, q).wait_recv()
        small += small_recv[q]
    small_dp[...] = small

    def small_dp_copy(peer, slot):
        return copy(small_dp, small_dp_recv.at[slot], smd_s.at[peer], smd_r.at[slot], peer, s)

    for k in range(1, D):
        small_dp_copy(lax.rem(d + k, D), d).start()

    backt[...] = dense_transposed(back_acc[...])
    scatter(down)
    dp_stage(up)

    small = small_dp[...]
    for k in range(1, D):
        e = lax.rem(d + k, D)
        small_dp_copy(e, e).wait_recv()
        small += small_dp_recv[e]
    groups = F // LANES
    factor = F32(cfg["tokens"]) / small[groups:groups + 1, 0:1]
    small_fin[...] = small * factor

    def small_ag_copy(peer, slot):
        return copy(small_fin, small_ag.at[slot], sma_s.at[peer], sma_r.at[slot], d, peer)

    for k in range(1, S):
        small_ag_copy(lax.rem(s + k, S), s).start()

    dp_stage(down)
    gather(up, factor)
    gather(down, factor)

    def put_gain(q, value):
        for j in range(groups):
            cols = pl.ds(pl.multiple_of(q * F + j * LANES, LANES), LANES)
            gain_ref[:, cols] = value[j:j + 1, :]

    put_gain(s, small_fin[...])
    for k in range(1, S):
        q = lax.rem(s + k, S)
        small_ag_copy(q, q).wait_recv()
        put_gain(q, small_ag[q])
    for b in (up, down):
        for k in range(1, S):
            q = lax.rem(s + k, S)
            ag_copy(b, q, q).wait_recv()
            cols = pl.ds(pl.multiple_of(q * b["width"], LANES), b["width"])
            b["out"][:, cols] = b["ag"][q].astype(F32)[0:R]

    for k in range(1, D):
        e = lax.rem(d + k, D)
        adapt_copy(e, d).wait_send()
        relay_copy(e, c).wait_send()
        small_dp_copy(e, d).wait_send()
        for b in (up, down):
            dp_copy(b, e, d).wait_send()
    for k in range(1, S):
        q = lax.rem(s + k, S)
        cot_copy(q, s).wait_send()
        small_copy(q, s).wait_send()
        small_ag_copy(q, s).wait_send()
        for b in (up, down):
            ag_copy(b, q, s).wait_send()
    for b in (up, down):
        d2d_copy(b, chip).wait_send()
        for j in range(1, K):
            k = lax.rem(chip + j, K)
            d2d_copy(b, k).wait_send()
            rs_copy(b, k, chip).wait_send()


def shards(projections, rotated_query_gradient, gains, adapter_lowering, adapter_raising,
           activations, positions, valid):
    D, S = lax.axis_size("dp"), lax.axis_size("seq")
    T, QF = projections.shape[2:]
    F = rotated_query_gradient.shape[3]
    R, M = adapter_lowering.shape[1:]
    W = -(-M // (LANES * S)) * LANES
    RP = -(-R // 16) * 16
    LH, UH = M // 2, QF // 2
    K = S // 2
    ranks = D * R
    cfg = dict(S=S, D=D, T=T, F=F, W=W, R=R, RP=RP, LH=LH, M=M, QF=QF, tokens=D * S * T)

    low, rai = adapter_lowering[0], adapter_raising[0]
    adapt = jnp.stack(
        [jnp.concatenate([low[:, h * LH:(h + 1) * LH], rai[:, h * UH:(h + 1) * UH]], 1) for h in range(2)]
    )
    adapt = jnp.pad(adapt, ((0, 0), (0, RP - R), (0, 0)))

    def stage(width):
        return [
            pltpu.VMEM((K, ranks, width), BF),
            pltpu.VMEM((K, ranks, width), BF),
            pltpu.VMEM((K, ranks, width), F32),
            pltpu.VMEM((K, ranks, width), BF),
            pltpu.VMEM((K, ranks, width), BF),
            pltpu.VMEM((ranks + RP, width), F32),
            pltpu.VMEM((D, RP, width), BF),
            pltpu.VMEM((D, RP, width), F32),
            pltpu.VMEM((D, RP, width), BF),
            pltpu.VMEM((S, RP, width), BF),
            pltpu.VMEM((RP, width), BF),
        ]

    hw = 256 if F % 256 == 0 else 128
    dma = pltpu.SemaphoreType.DMA
    any_space = pl.BlockSpec(memory_space=pl.ANY)
    vmem = pl.BlockSpec(memory_space=pltpu.VMEM)
    small_rows = -(-(F // LANES + 1) // 8) * 8
    down, up, gain = pl.pallas_call(
        functools.partial(kernel, cfg),
        out_shape=(
            jax.ShapeDtypeStruct((R, S * W), F32),
            jax.ShapeDtypeStruct((R, QF), F32),
            jax.ShapeDtypeStruct((1, QF), F32),
        ),
        in_specs=[any_space] * 4 + [vmem] * 4,
        out_specs=(vmem, vmem, vmem),
        scratch_shapes=[
            pltpu.VMEM((T, QF), BF),
            pltpu.VMEM((T, S * W), BF),
            pltpu.VMEM((S, T, F), BF),
            pltpu.VMEM((D, 2, RP, LH + UH), BF),
            pltpu.VMEM((S, T, F), F32),
            pltpu.VMEM((T, D * RP), F32),
            pltpu.VMEM((T, LANES), F32),
            pltpu.VMEM((T, LANES), F32),
            pltpu.VMEM((T, hw), F32),
            pltpu.VMEM((T, hw), F32),
            pltpu.VMEM((ranks, T), BF),
            pltpu.VMEM((ranks, T), BF),
            pltpu.VMEM((S, small_rows, LANES), F32),
            pltpu.VMEM((S, small_rows, LANES), F32),
            pltpu.VMEM((small_rows, LANES), F32),
            pltpu.VMEM((D, small_rows, LANES), F32),
            pltpu.VMEM((small_rows, LANES), F32),
            pltpu.VMEM((S, small_rows, LANES), F32),
        ]
        + stage(F)
        + stage(W)
        + [dma((4,)), dma((S,)), dma((S,)), dma((D,)), dma((D,)), dma((D,)), dma((D,))]
        + [dma((S,)), dma((S,)), dma((D,)), dma((D,)), dma((S,)), dma((S,))]
        + [dma((2, K)), dma((2, K)), dma((2, K)), dma((2, K))]
        + [dma((2, D)), dma((2, D)), dma((2, S)), dma((2, S))],
        compiler_params=pltpu.CompilerParams(
            collective_id=0, has_side_effects=True, vmem_limit_bytes=56 * 1024 * 1024
        ),
    )(
        projections.reshape(T, QF),
        rotated_query_gradient.reshape(S, T, F),
        activations.reshape(T, M),
        adapt,
        gains,
        jnp.asarray(lane_frequencies()),
        positions.reshape(3, T),
        valid.reshape(1, T),
    )
    return down[None, :, :M], up[None], gain


def solution(mesh):
    in_specs = (
        P(None, "dp", "seq", None),
        P(None, "dp", None, "seq"),
        P(),
        P(None, "dp", None),
        P(None, "dp", None),
        P("dp", "seq", None),
        P(None, "dp", "seq"),
        P("dp", "seq"),
    )
    out_specs = (P(None, "dp", None), P(None, "dp", None), P())
    return jax.shard_map(shards, mesh=mesh, in_specs=in_specs, out_specs=out_specs, check_vma=False)
```

```python
import functools

import jax
import jax.numpy as jnp
import numpy as np
from jax import lax
from jax.experimental import pallas as pl
from jax.experimental.pallas import tpu as pltpu
from jax.sharding import PartitionSpec as P

HD = 128
EPSILON = 1e-06
LANES = 128
BF = jnp.bfloat16
F32 = jnp.float32
MESH = pl.DeviceIdType.MESH
NT = (((1,), (1,)), ((), ()))


def group_counts():
    one_sixth = HD // 6
    return (HD // 2 - 2 * one_sixth, one_sixth, one_sixth)


def lane_frequencies():
    pieces = []
    for n in group_counts():
        pieces.append(np.float32(10000.0) ** (-np.arange(n, dtype=np.float32) / np.float32(n)))
    return np.repeat(np.concatenate(pieces).astype(np.float32), 2)[None]


def kernel(
    cfg,
    proj_hbm, cot_hbm, act_hbm, low_hbm, rai_hbm, gains_ref, freq_ref, pos_ref, valid_ref,
    down_ref, up_ref, gain_ref,
    proj, act, cot, cot_src, low, rai, fold, packed, adapt, scaled, back_acc, dot_acc, inv_ref, cos_ref, sin_ref, redt, backt,
    small_send, small_recv, small_dp, small_dp_recv, small_fin, small_ag,
    d2d_send_u, d2d_recv_u, own_u, rs_send_u, rs_recv_u, tot_u, dp_send_u, dp_f_u, dp_recv_u, ag_u, fin_u,
    d2d_send_d, d2d_recv_d, own_d, rs_send_d, rs_recv_d, tot_d, dp_send_d, dp_f_d, dp_recv_d, ag_d, fin_d,
    local_sem, cot_s, cot_r, ad_s, ad_r, rel_s, rel_r,
    sm_s, sm_r, smd_s, smd_r, sma_s, sma_r,
    d2d_s, d2d_r, rs_s, rs_r, dp_s, dp_r, ag_s, ag_r,
):
    S, D, T, F, W, R, RP, LH, UH, M, QF, fd = (
        cfg[k] for k in ("S", "D", "T", "F", "W", "R", "RP", "LH", "UH", "M", "QF", "fd")
    )
    K = S // 2
    ranks = D * R
    hw = 256 if F % 256 == 0 else 128
    d = lax.axis_index("dp")
    s = lax.axis_index("seq")
    c = lax.rem(s, 2)
    chip = s // 2
    sib = s + 1 - 2 * c

    def copy(src, dst, ss, rs, dp, seq):
        return pltpu.make_async_remote_copy(
            src_ref=src, dst_ref=dst, send_sem=ss, recv_sem=rs,
            device_id=(dp, seq), device_id_type=MESH,
        )

    loads = [
        pltpu.make_async_copy(proj_hbm, proj, local_sem.at[0]),
        pltpu.make_async_copy(act_hbm, act.at[:, pl.ds(0, M)], local_sem.at[1]),
        pltpu.make_async_copy(cot_hbm, cot_src, local_sem.at[2]),
        pltpu.make_async_copy(low_hbm, low, local_sem.at[3]),
        pltpu.make_async_copy(rai_hbm, rai, local_sem.at[4]),
    ]
    for i in (3, 4, 2, 0, 1):
        loads[i].start()

    barrier = pltpu.get_barrier_semaphore()
    for k in range(1, S):
        pl.semaphore_signal(barrier, inc=1, device_id=(d, lax.rem(s + k, S)), device_id_type=MESH)
    for k in range(1, D):
        pl.semaphore_signal(barrier, inc=1, device_id=(lax.rem(d + k, D), s), device_id_type=MESH)

    LF, UF = LH // fd, UH // fd
    fold[...] = jnp.zeros_like(fold)
    loads[3].wait()
    loads[4].wait()
    for h in range(2):
        for q in range(fd):
            fold[q * R:(q + 1) * R, 0:LF] = low[:, h * LH + q * LF:h * LH + (q + 1) * LF].astype(F32)
            fold[q * R:(q + 1) * R, LF:LF + UF] = rai[:, h * UH + q * UF:h * UH + (q + 1) * UF].astype(F32)
        packed[d, h] = fold[0:packed.shape[2], :].astype(BF)

    loads[2].wait()
    pl.semaphore_wait(barrier, S + D - 2)

    def cot_copy(peer, slot):
        return copy(cot_src.at[peer], cot.at[slot], cot_s.at[peer], cot_r.at[slot], d, peer)

    def adapt_copy(peer, slot):
        return copy(packed.at[d, c], packed.at[slot, c], ad_s.at[peer], ad_r.at[slot], peer, s)

    def relay_copy(slot, half):
        return copy(packed.at[slot, half], packed.at[slot, half], rel_s.at[slot], rel_r.at[slot], d, sib)

    for k in range(1, D):
        adapt_copy(lax.rem(d + k, D), d).start()
    for k in range(1, S):
        cot_copy(lax.rem(s + k, S), s).start()

    n0, n1, _ = group_counts()
    lane = lax.broadcasted_iota(jnp.int32, (T, LANES), 1)

    def column(row):
        return jnp.broadcast_to(row.astype(F32), (LANES, T)).T

    index = jnp.where(
        lane < 2 * n0, column(pos_ref[0]),
        jnp.where(lane < 2 * (n0 + n1), column(pos_ref[1]), column(pos_ref[2])),
    )
    angle = index * freq_ref[...]
    ok = column(valid_ref[...])
    co = jnp.cos(angle) * ok
    si = jnp.sin(angle) * ok
    for i in range(hw // LANES):
        cos_ref[:, i * LANES:(i + 1) * LANES] = co
        sin_ref[:, i * LANES:(i + 1) * LANES] = si
    row_i = lax.broadcasted_iota(jnp.int32, (hw, hw), 0)
    col_i = lax.broadcasted_iota(jnp.int32, (hw, hw), 1)
    even = lax.rem(col_i, 2) == 0
    swap = jnp.where(
        even & (row_i == col_i + 1), 1.0, jnp.where(jnp.logical_not(even) & (row_i == col_i - 1), -1.0, 0.0)
    ).astype(BF)
    count = jnp.sum(valid_ref[...].astype(F32), axis=1, keepdims=True)
    small_send[...] = jnp.broadcast_to(count[:, :, None], small_send.shape)

    loads[0].wait()
    square = jnp.zeros((T, LANES), F32)
    for i in range(QF // LANES):
        v = proj[:, i * LANES:(i + 1) * LANES].astype(F32)
        square += v * v
    inverse = lax.rsqrt(jnp.sum(square, axis=1, keepdims=True) / QF + EPSILON)
    inv_ref[...] = jnp.broadcast_to(inverse, (T, LANES))
    dot_acc[...] = jnp.zeros_like(dot_acc)

    def wide(x):
        return jnp.concatenate([x] * (hw // LANES), axis=1) if hw > LANES else x

    def chunk(p, source=cot):
        inv = wide(inv_ref[...])
        cw, sw = cos_ref[...], sin_ref[...]
        for i in range(F // hw):
            cols = pl.ds(pl.multiple_of(p * F + i * hw, LANES), hw)
            x = source[p, :, i * hw:(i + 1) * hw]
            xs = jnp.dot(x, swap, preferred_element_type=F32)
            un = cw * x.astype(F32) + sw * xs
            prod = un * (proj[:, cols].astype(F32) * inv)
            g = jnp.sum(prod, axis=0, keepdims=True)
            for t in range(hw // LANES):
                j = i * (hw // LANES) + t
                small_send[p, j:j + 1, :] = g[:, t * LANES:(t + 1) * LANES]
            gn = gains_ref[:, cols]
            scaled[p, :, i * hw:(i + 1) * hw] = un * gn
            pg = prod * gn
            acc = pg[:, :LANES]
            for t in range(1, hw // LANES):
                acc += pg[:, t * LANES:(t + 1) * LANES]
            dot_acc[...] += acc

    chunk(s, cot_src)
    cot_copy(sib, sib).wait_recv()
    chunk(sib)

    def rest(j, carry):
        p = lax.rem(2 * chip + 2 + j, S)
        cot_copy(p, p).wait_recv()
        chunk(p)
        return carry

    half_rest = (S - 2) // 2
    lax.fori_loop(0, half_rest, rest, 0)
    for k in range(1, D):
        e = lax.rem(d + k, D)
        adapt_copy(e, e).wait_recv()
        relay_copy(e, c).start()
    lax.fori_loop(half_rest, S - 2, rest, 0)

    def small_copy(peer, slot):
        return copy(small_send.at[peer], small_recv.at[slot], sm_s.at[peer], sm_r.at[slot], d, peer)

    for k in range(1, S):
        small_copy(lax.rem(s + k, S), s).start()

    r_i = lax.broadcasted_iota(jnp.int32, (ranks, D * RP), 0)
    q_i = lax.broadcasted_iota(jnp.int32, (ranks, D * RP), 1)
    pick = jnp.where(q_i == (r_i // R) * RP + lax.rem(r_i, R), 1.0, 0.0).astype(BF)

    def dense_transposed(x):
        return lax.dot_general(pick, x.astype(BF), NT, preferred_element_type=F32).astype(BF)

    for k in range(1, D):
        e = lax.rem(d + k, D)
        relay_copy(e, 1 - c).wait_recv()

    def unfold(e, carry):
        for h in range(2):
            fold[0:packed.shape[2], :] = packed[e, h].astype(F32)
            for q in range(fd):
                rows = fold[q * R:q * R + RP, :].astype(BF)
                adapt[e, h, :, q * LF:(q + 1) * LF] = rows[:, 0:LF]
                adapt[e, h, :, LH + q * UF:LH + (q + 1) * UF] = rows[:, LF:LF + UF]
        return carry

    lax.fori_loop(0, D, unfold, 0)
    loads[1].wait()
    red = jnp.zeros((T, D * RP), F32)
    for h in range(2):
        lowering = adapt[:, h, :, 0:LH].reshape(D * RP, LH)
        red += lax.dot_general(act[:, h * LH:(h + 1) * LH], lowering, NT, preferred_element_type=F32)
    redt[...] = dense_transposed(red)

    back_acc[...] = jnp.zeros_like(back_acc)
    dot_mean = jnp.sum(dot_acc[...], axis=1, keepdims=True) / QF
    mean_w = jnp.broadcast_to(dot_mean, (T, LANES))
    dot_acc[...] = mean_w

    def up_term(p):
        inv = wide(inv_ref[...])
        mean = wide(dot_acc[...])
        parts = []
        for i in range(F // hw):
            cols = pl.ds(pl.multiple_of(p * F + i * hw, LANES), hw)
            nrm = proj[:, cols].astype(F32) * inv
            parts.append((inv * (scaled[p, :, i * hw:(i + 1) * hw] - nrm * mean)).astype(BF))
        delta = jnp.concatenate(parts, axis=1) if len(parts) > 1 else parts[0]
        h = p // K
        off = pl.multiple_of(LH + lax.rem(p, K) * F, LANES)
        raising = adapt[:, h, :, pl.ds(off, F)].reshape(D * RP, F)
        back_acc[...] += lax.dot_general(delta, raising, NT, preferred_element_type=F32)
        return jnp.dot(redt[...], delta, preferred_element_type=F32)

    def down_term(p):
        cols = pl.ds(pl.multiple_of(p * W, LANES), W)
        return jnp.dot(backt[...], act[:, cols], preferred_element_type=F32)

    up = dict(i=0, term=up_term, d2d_send=d2d_send_u, d2d_recv=d2d_recv_u, own=own_u,
              rs_send=rs_send_u, rs_recv=rs_recv_u, tot=tot_u, dp_send=dp_send_u, dp_f=dp_f_u,
              dp_recv=dp_recv_u, ag=ag_u, fin=fin_u, out=up_ref, width=F)
    down = dict(i=1, term=down_term, d2d_send=d2d_send_d, d2d_recv=d2d_recv_d, own=own_d,
                rs_send=rs_send_d, rs_recv=rs_recv_d, tot=tot_d, dp_send=dp_send_d, dp_f=dp_f_d,
                dp_recv=dp_recv_d, ag=ag_d, fin=fin_d, out=down_ref, width=W)

    def d2d_copy(b, k):
        i = b["i"]
        return copy(b["d2d_send"].at[k], b["d2d_recv"].at[k], d2d_s.at[i, k], d2d_r.at[i, k], d, sib)

    def rs_copy(b, peer, slot):
        i = b["i"]
        return copy(b["rs_send"].at[peer], b["rs_recv"].at[slot], rs_s.at[i, peer], rs_r.at[i, slot],
                    d, 2 * peer + c)

    def dp_copy(b, peer, slot):
        i = b["i"]
        return copy(b["dp_send"].at[peer], b["dp_recv"].at[slot], dp_s.at[i, peer], dp_r.at[i, slot],
                    peer, s)

    def ag_copy(b, peer, slot):
        i = b["i"]
        return copy(b["fin"], b["ag"].at[slot], ag_s.at[i, peer], ag_r.at[i, slot], d, peer)

    def scatter(b):
        def for_sibling(j, carry):
            k = lax.rem(chip + 1 + j, K)
            b["d2d_send"][k] = b["term"](2 * k + 1 - c).astype(BF)
            d2d_copy(b, k).start()
            return carry

        def for_this_core(j, carry):
            k = lax.rem(chip + 1 + j, K)
            b["own"][k] = b["term"](2 * k + c)
            return carry

        lax.fori_loop(0, K, for_sibling, 0)
        lax.fori_loop(0, K, for_this_core, 0)
        for j in range(1, K):
            k = lax.rem(chip + j, K)
            d2d_copy(b, k).wait_recv()
            b["rs_send"][k] = (b["own"][k] + b["d2d_recv"][k].astype(F32)).astype(BF)
            rs_copy(b, k, chip).start()

    def dp_stage(b):
        d2d_copy(b, chip).wait_recv()
        total = b["own"][chip] + b["d2d_recv"][chip].astype(F32)
        for j in range(1, K):
            q = lax.rem(chip + j, K)
            rs_copy(b, q, q).wait_recv()
            total += b["rs_recv"][q].astype(F32)
        b["tot"][0:ranks, :] = total
        for e in range(D):
            rows = b["tot"][e * R:e * R + RP, :]
            b["dp_f"][e] = rows
            b["dp_send"][e] = rows.astype(BF)
        for k in range(1, D):
            dp_copy(b, lax.rem(d + k, D), d).start()

    def gather(b, factor):
        total = b["dp_f"][d]
        for k in range(1, D):
            e = lax.rem(d + k, D)
            dp_copy(b, e, e).wait_recv()
            total += b["dp_recv"][e].astype(F32)
        fin = (total * factor).astype(BF)
        b["fin"][...] = fin
        for k in range(1, S):
            ag_copy(b, lax.rem(s + k, S), s).start()
        cols = pl.ds(pl.multiple_of(s * b["width"], LANES), b["width"])
        b["out"][:, cols] = fin.astype(F32)[0:R]

    scatter(up)

    small = small_send[s]
    for k in range(1, S):
        q = lax.rem(s + k, S)
        small_copy(q, q).wait_recv()
        small += small_recv[q]
    small_dp[...] = small

    def small_dp_copy(peer, slot):
        return copy(small_dp, small_dp_recv.at[slot], smd_s.at[peer], smd_r.at[slot], peer, s)

    for k in range(1, D):
        small_dp_copy(lax.rem(d + k, D), d).start()

    backt[...] = dense_transposed(back_acc[...])
    scatter(down)
    dp_stage(up)

    small = small_dp[...]
    for k in range(1, D):
        e = lax.rem(d + k, D)
        small_dp_copy(e, e).wait_recv()
        small += small_dp_recv[e]
    groups = F // LANES
    factor = F32(cfg["tokens"]) / small[groups:groups + 1, 0:1]
    small_fin[...] = small * factor

    def small_ag_copy(peer, slot):
        return copy(small_fin, small_ag.at[slot], sma_s.at[peer], sma_r.at[slot], d, peer)

    for k in range(1, S):
        small_ag_copy(lax.rem(s + k, S), s).start()

    dp_stage(down)
    gather(up, factor)
    gather(down, factor)

    def put_gain(q, value):
        for j in range(groups):
            cols = pl.ds(pl.multiple_of(q * F + j * LANES, LANES), LANES)
            gain_ref[:, cols] = value[j:j + 1, :]

    put_gain(s, small_fin[...])
    for k in range(1, S):
        q = lax.rem(s + k, S)
        small_ag_copy(q, q).wait_recv()
        put_gain(q, small_ag[q])
    for b in (up, down):
        for k in range(1, S):
            q = lax.rem(s + k, S)
            ag_copy(b, q, q).wait_recv()
            cols = pl.ds(pl.multiple_of(q * b["width"], LANES), b["width"])
            b["out"][:, cols] = b["ag"][q].astype(F32)[0:R]

    for k in range(1, D):
        e = lax.rem(d + k, D)
        adapt_copy(e, d).wait_send()
        relay_copy(e, c).wait_send()
        small_dp_copy(e, d).wait_send()
        for b in (up, down):
            dp_copy(b, e, d).wait_send()
    for k in range(1, S):
        q = lax.rem(s + k, S)
        cot_copy(q, s).wait_send()
        small_copy(q, s).wait_send()
        small_ag_copy(q, s).wait_send()
        for b in (up, down):
            ag_copy(b, q, s).wait_send()
    for b in (up, down):
        d2d_copy(b, chip).wait_send()
        for j in range(1, K):
            k = lax.rem(chip + j, K)
            d2d_copy(b, k).wait_send()
            rs_copy(b, k, chip).wait_send()


def place(down_ref, up_ref, gain_ref, down_out, up_out, gain_out):
    for r in range(down_out.shape[0]):
        down_out[r] = down_ref[r:r + 1, 0:down_out.shape[2]]
        up_out[r] = up_ref[r:r + 1, :]
    gain_out[...] = gain_ref[...]


def shards(projections, rotated_query_gradient, gains, adapter_lowering, adapter_raising,
           activations, positions, valid):
    D, S = lax.axis_size("dp"), lax.axis_size("seq")
    T, QF = projections.shape[2:]
    F = rotated_query_gradient.shape[3]
    R, M = adapter_lowering.shape[1:]
    W = -(-M // (LANES * S)) * LANES
    RP = -(-R // 16) * 16
    LH, UH = M // 2, QF // 2
    K = S // 2
    ranks = D * R
    fd = 4 if R % 4 == 0 and LH % (4 * LANES) == 0 and UH % (4 * LANES) == 0 else 1
    folded = -(-fd * R // 16) * 16
    cfg = dict(S=S, D=D, T=T, F=F, W=W, R=R, RP=RP, LH=LH, UH=UH, M=M, QF=QF, fd=fd, tokens=D * S * T)

    def stage(width):
        return [
            pltpu.VMEM((K, ranks, width), BF),
            pltpu.VMEM((K, ranks, width), BF),
            pltpu.VMEM((K, ranks, width), F32),
            pltpu.VMEM((K, ranks, width), BF),
            pltpu.VMEM((K, ranks, width), BF),
            pltpu.VMEM((ranks + RP, width), F32),
            pltpu.VMEM((D, RP, width), BF),
            pltpu.VMEM((D, RP, width), F32),
            pltpu.VMEM((D, RP, width), BF),
            pltpu.VMEM((S, RP, width), BF),
            pltpu.VMEM((RP, width), BF),
        ]

    hw = 256 if F % 256 == 0 else 128
    dma = pltpu.SemaphoreType.DMA
    any_space = pl.BlockSpec(memory_space=pl.ANY)
    vmem = pl.BlockSpec(memory_space=pltpu.VMEM)
    small_rows = -(-(F // LANES + 1) // 8) * 8
    down, up, gain = pl.pallas_call(
        functools.partial(kernel, cfg),
        out_shape=(
            jax.ShapeDtypeStruct((R, S * W), F32),
            jax.ShapeDtypeStruct((R, QF), F32),
            jax.ShapeDtypeStruct((1, QF), F32),
        ),
        in_specs=[any_space] * 5 + [vmem] * 4,
        out_specs=(vmem, vmem, vmem),
        scratch_shapes=[
            pltpu.VMEM((T, QF), BF),
            pltpu.VMEM((T, S * W), BF),
            pltpu.VMEM((S, T, F), BF),
            pltpu.VMEM((S, T, F), BF),
            pltpu.VMEM((R, M), BF),
            pltpu.VMEM((R, QF), BF),
            pltpu.VMEM((folded + 16, (LH + UH) // fd), F32),
            pltpu.VMEM((D, 2, folded, (LH + UH) // fd), BF),
            pltpu.VMEM((D, 2, RP, LH + UH), BF),
            pltpu.VMEM((S, T, F), F32),
            pltpu.VMEM((T, D * RP), F32),
            pltpu.VMEM((T, LANES), F32),
            pltpu.VMEM((T, LANES), F32),
            pltpu.VMEM((T, hw), F32),
            pltpu.VMEM((T, hw), F32),
            pltpu.VMEM((ranks, T), BF),
            pltpu.VMEM((ranks, T), BF),
            pltpu.VMEM((S, small_rows, LANES), F32),
            pltpu.VMEM((S, small_rows, LANES), F32),
            pltpu.VMEM((small_rows, LANES), F32),
            pltpu.VMEM((D, small_rows, LANES), F32),
            pltpu.VMEM((small_rows, LANES), F32),
            pltpu.VMEM((S, small_rows, LANES), F32),
        ]
        + stage(F)
        + stage(W)
        + [dma((5,)), dma((S,)), dma((S,)), dma((D,)), dma((D,)), dma((D,)), dma((D,))]
        + [dma((S,)), dma((S,)), dma((D,)), dma((D,)), dma((S,)), dma((S,))]
        + [dma((2, K)), dma((2, K)), dma((2, K)), dma((2, K))]
        + [dma((2, D)), dma((2, D)), dma((2, S)), dma((2, S))],
        compiler_params=pltpu.CompilerParams(
            collective_id=0, has_side_effects=True, vmem_limit_bytes=56 * 1024 * 1024
        ),
    )(
        projections.reshape(T, QF),
        rotated_query_gradient.reshape(S, T, F),
        activations.reshape(T, M),
        adapter_lowering[0],
        adapter_raising[0],
        gains,
        jnp.asarray(lane_frequencies()),
        positions,
        valid.reshape(1, T),
    )
    down, up, gain = pl.pallas_call(
        place,
        out_shape=(
            jax.ShapeDtypeStruct((R, 1, M), F32),
            jax.ShapeDtypeStruct((R, 1, QF), F32),
            jax.ShapeDtypeStruct((1, QF), F32),
        ),
        in_specs=[vmem] * 3,
        out_specs=(vmem, vmem, vmem),
    )(down, up, gain)
    return down.reshape(1, R, M), up.reshape(1, R, QF), gain


def solution(mesh):
    in_specs = (
        P(None, "dp", "seq", None),
        P(None, "dp", None, "seq"),
        P(),
        P(None, "dp", None),
        P(None, "dp", None),
        P("dp", "seq", None),
        P(None, "dp", "seq"),
        P("dp", "seq"),
    )
    out_specs = (P(None, "dp", None), P(None, "dp", None), P())
    return jax.shard_map(shards, mesh=mesh, in_specs=in_specs, out_specs=out_specs, check_vma=False)
```
